32 devices in a mesh: pipe: 2 (over x), tensor: 4 (over y, core), seq: 4 (over z).
Axes of the slice: x: 2, y: 2, z: 4, core: 2. Of those that a mesh axis runs over, the one named last changes fastest.
Arguments:
- tokens: bfloat16 [2, 512, 2560], P(None, 'seq', 'tensor'), may hold values from -6 to 6
- prenorm_gain: float32 [2, 2560], P('pipe'), may hold values from 0.5 to 1.5
- gate_weight: bfloat16 [2, 2560, 5120], P('pipe', None, 'tensor'), may hold values from -0.125 to 0.125
- inner_weight: bfloat16 [2, 2560, 5120], P('pipe', None, 'tensor'), may hold values from -0.125 to 0.125
- state_weight: bfloat16 [2, 2560, 256], P('pipe'), may hold values from -0.125 to 0.125
- step_weight: bfloat16 [2, 2560, 80], P('pipe', None, 'tensor'), may hold values from -0.125 to 0.125
- inner_taps: float32 [2, 5, 5120], P('pipe', None, 'tensor'), may hold values from -3 to 3
- state_taps: float32 [2, 5, 256], P('pipe'), may hold values from -3 to 3
- step_bias: float32 [2, 80], P('pipe', 'tensor'), may hold values from -5 to -2
- decay_rate: float32 [2, 80], P('pipe', 'tensor'), may hold values from 0.001953125 to 1
- skip_scale: float32 [2, 80], P('pipe', 'tensor'), may hold values from 0.5 to 1.5
- inner_gain: float32 [2, 5120], P('pipe', 'tensor'), may hold values from 0.5 to 1.5
- out_weight: bfloat16 [2, 5120, 2560], P('pipe', 'tensor'), may hold values from -0.078125 to 0.078125
Outputs:
- layer_outputs: bfloat16 [2, 2, 512, 2560], P('pipe', None, 'seq', 'tensor')
The draws below stay inside these ranges and needn't reach their ends.
All inputs are finite; a program needn't handle non-finite values.
Results may differ from the reference program's by a relative error of at most 0.019.
Values may be sent and summed in bfloat16 or wider, within the bound.
A program may use at most 64 MiB of HBM per device.

```python
import math
import jax
import jax.numpy as jnp
from jax import lax

D = 2560
HEADS = 80
HEADDIM = 64
STATE = 128
KW = 4
BLOCK = 128
MICRO = 2
INNER = 5120
TOKENS = 512
LAYERS = 2


def block_levels(own_key, extent, cuts, least, top_value):
    level, own = 1.0, jax.random.fold_in(own_key, 6)
    for position, shards_of in cuts:
        steps = jnp.exp(jax.random.uniform(jax.random.fold_in(own, position), (shards_of,), jnp.float32, least / len(cuts), top_value / len(cuts)))
        level = level * jnp.repeat(steps, extent[position] // shards_of).reshape([-1 if axis == position else 1 for axis in range(len(extent))])
    return level


def gaussian(own_key, shape, scale, bound, shards=(), held_as=jnp.bfloat16):
    values = scale * jax.random.normal(own_key, shape, jnp.float32)
    if shards:
        values = values * block_levels(own_key, shape, shards, -0.22, 0.18)
    return jnp.clip(values, -bound, bound).astype(held_as)


def setup_inputs(seed: int = 0) -> dict:
    splits = jax.random.split(jax.random.key(seed), 14)
    return {
        "tokens": gaussian(splits[0], (MICRO, TOKENS, D), 1.0, 6.0, ((1, 4), (2, 4))),
        "prenorm_gain": jnp.clip(1.0 + 0.1 * jax.random.normal(splits[1], (LAYERS, D), jnp.float32), 0.5, 1.5),
        "gate_weight": gaussian(splits[2], (LAYERS, D, INNER), D ** -0.5, 0.125, ((0, 2), (2, 4))),
        "inner_weight": gaussian(splits[3], (LAYERS, D, INNER), D ** -0.5, 0.125, ((0, 2), (2, 4))),
        "state_weight": gaussian(splits[4], (LAYERS, D, 2 * STATE), D ** -0.5, 0.125, ((0, 2),)),
        "step_weight": gaussian(splits[5], (LAYERS, D, HEADS), D ** -0.5, 0.125, ((0, 2), (2, 4))),
        "inner_taps": gaussian(splits[6], (LAYERS, KW + 1, INNER), 0.5, 3.0, ((0, 2), (2, 4)), jnp.float32),
        "state_taps": gaussian(splits[7], (LAYERS, KW + 1, 2 * STATE), 0.5, 3.0, ((0, 2),), jnp.float32),
        "step_bias": jnp.clip(-5.0 + 3.0 * jax.random.uniform(splits[8], (LAYERS, HEADS), jnp.float32) ** block_levels(splits[8], (LAYERS, HEADS), ((0, 2), (1, 4)), -0.2, 0.2), -5.0, -2.0),
        "decay_rate": jnp.clip(jnp.exp(math.log(1.0) - 6.2383246 * jax.random.uniform(splits[9], (LAYERS, HEADS), jnp.float32) ** block_levels(splits[9], (LAYERS, HEADS), ((0, 2), (1, 4)), -0.2, 0.2)), 0.001953125, 1.0),
        "skip_scale": jnp.clip(0.5 + 1.0 * jax.random.uniform(splits[10], (LAYERS, HEADS), jnp.float32) ** block_levels(splits[10], (LAYERS, HEADS), ((0, 2), (1, 4)), -0.2, 0.2), 0.5, 1.5),
        "inner_gain": jnp.clip(1.0 + 0.1 * jax.random.normal(splits[11], (LAYERS, INNER), jnp.float32), 0.5, 1.5),
        "out_weight": gaussian(splits[12], (LAYERS, INNER, D), INNER ** -0.5, 0.078125, ((0, 2), (1, 4))),
    }


EPS = 1e-05

def causal_taps(values, taps):
    width = taps.shape[0] - 1
    length = values.shape[0]
    zeros = jnp.zeros((width - 1, values.shape[1]), values.dtype)
    padded = jnp.concatenate([zeros, values], axis=0).astype(jnp.float32)
    total = jnp.broadcast_to(taps[width][None, :], (length, values.shape[1]))
    for index in range(width):
        total = total + taps[index][None, :] * padded[index:index + length]
    return jax.nn.silu(total).astype(jnp.bfloat16)

def block_terms(inner_block, input_block, output_block, step_block, rate):
    size = step_block.shape[0]
    cumulative = jnp.cumsum(-step_block * rate[None, :], axis=0)
    by_head = cumulative.T
    later = jnp.arange(size)[:, None] >= jnp.arange(size)[None, :]
    decay = jnp.exp(jnp.where(later[None], by_head[:, :, None] - by_head[:, None, :], -jnp.inf))
    scores = jnp.dot(output_block, input_block.T, preferred_element_type=jnp.float32)
    mixing = (scores[None] * decay * step_block.T[:, None, :]).astype(jnp.bfloat16)
    inside = jnp.einsum('hqs,shp->qhp', mixing.astype(jnp.float32), inner_block.astype(jnp.float32))
    weighting = jnp.exp(cumulative[-1:] - cumulative) * step_block
    weighted = (inner_block.astype(jnp.float32) * weighting[:, :, None]).astype(jnp.bfloat16)
    state = jnp.einsum('shp,sn->hpn', weighted.astype(jnp.float32), input_block.astype(jnp.float32))
    return (cumulative, inside, state, jnp.exp(cumulative[-1]))

def state_space(inner_conv, state_conv, step_size, rate, skip):
    length = inner_conv.shape[0]
    count = length // BLOCK
    inner_blocks = inner_conv.reshape(count, BLOCK, HEADS, HEADDIM)
    input_blocks = state_conv[:, :STATE].reshape(count, BLOCK, STATE)
    output_blocks = state_conv[:, STATE:].reshape(count, BLOCK, STATE)
    step_blocks = step_size.reshape(count, BLOCK, HEADS)

    def advance(carried, items):
        inner_block, input_block, output_block, step_block = items
        cumulative, inside, state, decay = block_terms(inner_block, input_block, output_block, step_block, rate)
        across = jnp.exp(cumulative)[:, :, None] * jnp.einsum('qn,hpn->qhp', output_block.astype(jnp.float32), carried, precision=lax.Precision.HIGHEST)
        return (carried * decay[:, None, None] + state, inside + across)
    initial = jnp.zeros((HEADS, HEADDIM, STATE), jnp.float32)
    _, pieces = lax.scan(advance, initial, (inner_blocks, input_blocks, output_blocks, step_blocks))
    mixed = pieces + skip[None, None, :, None] * inner_blocks.astype(jnp.float32)
    return mixed.reshape(length, HEADS * HEADDIM)

def layer(current, prenorm, gate_weight, inner_weight, state_weight, step_weight, inner_taps, state_taps, step_bias, decay_rate, skip_scale, inner_gain, out_weight):
    widened = current.astype(jnp.float32)
    normed_in = (widened * lax.rsqrt(lax.optimization_barrier(jnp.mean(widened * widened, axis=1, keepdims=True)) + EPS) * prenorm).astype(jnp.bfloat16)
    gate_raw = jnp.dot(normed_in, gate_weight, preferred_element_type=jnp.float32).astype(jnp.bfloat16)
    inner_raw = jnp.dot(normed_in, inner_weight, preferred_element_type=jnp.float32).astype(jnp.bfloat16)
    state_raw = jnp.dot(normed_in, state_weight, preferred_element_type=jnp.float32).astype(jnp.bfloat16)
    step_raw = jnp.dot(normed_in, step_weight, preferred_element_type=jnp.float32)
    inner_conv = causal_taps(inner_raw, inner_taps)
    state_conv = causal_taps(state_raw, state_taps)
    step_size = jax.nn.softplus(step_raw + step_bias)
    mixed = state_space(inner_conv, state_conv, step_size, decay_rate, skip_scale)
    gated = mixed * jax.nn.silu(gate_raw.astype(jnp.float32))
    normed = (gated * lax.rsqrt(lax.optimization_barrier(jnp.mean(gated * gated, axis=1, keepdims=True)) + EPS) * inner_gain).astype(jnp.bfloat16)
    summed = jnp.dot(normed, out_weight, preferred_element_type=jnp.float32)
    return (widened + summed).astype(jnp.bfloat16)

def reference(tokens, prenorm_gain, gate_weight, inner_weight, state_weight, step_weight, inner_taps, state_taps, step_bias, decay_rate, skip_scale, inner_gain, out_weight):
    results = []
    for micro in range(MICRO):
        current = tokens[micro]
        per_layer = []
        for depth in range(LAYERS):
            current = layer(current, prenorm_gain[depth], gate_weight[depth], inner_weight[depth], state_weight[depth], step_weight[depth], inner_taps[depth], state_taps[depth], step_bias[depth], decay_rate[depth], skip_scale[depth], inner_gain[depth], out_weight[depth])
            per_layer.append(current)
        results.append(jnp.stack(per_layer))
    return jnp.stack(results, axis=1)
```

```python
import functools

import jax
import jax.numpy as jnp
from jax import lax
from jax.experimental import pallas as pl
from jax.experimental.pallas import tpu as pltpu
from jax.sharding import PartitionSpec as P

EPS = 1e-05
LANES = 128
MESH = pl.DeviceIdType.MESH
F32 = jnp.float32
BF16 = jnp.bfloat16


def silu(v):
    return v / (1.0 + jnp.exp(-v))


def remote(src, dst, send, recv, where):
    return pltpu.make_async_remote_copy(
        src_ref=src, dst_ref=dst, send_sem=send, recv_sem=recv, device_id=where, device_id_type=MESH
    )


def kernel(
    sizes,
    tokens,
    prenorm,
    gate_hbm,
    inner_hbm,
    state_hbm,
    step_hbm,
    inner_taps,
    state_taps,
    step_bias,
    decay_rate,
    skip_scale,
    inner_gain,
    out_hbm,
    out,
    w_gate,
    w_inner,
    w_state,
    w_step,
    w_out,
    u,
    ni,
    raw,
    rim,
    taps,
    conv,
    gate,
    steps,
    rates,
    cum_t,
    step_t,
    b_t,
    scores,
    states,
    ent,
    snd,
    g,
    sq_acc,
    sq_own,
    sq_all,
    term,
    parts,
    own,
    w_sem,
    ag_send,
    ag_recv,
    rim_send,
    rim_recv,
    ch_send,
    ch_recv,
    rs_send,
    rs_recv,
    sq_send,
    sq_recv,
    pipe_send,
    pipe_recv,
):
    n_pipe, n_tensor, n_seq = sizes
    micros, rows, narrow = own.shape
    width = prenorm.shape[1]
    inner = w_inner.shape[1]
    heads = step_bias.shape[1]
    head_size = inner // heads
    pack = LANES // head_size
    pairs = inner // LANES
    tiles = raw.shape[2] // LANES
    reach = inner_taps.shape[1] - 2
    edge = rim.shape[1]
    section = lax.axis_index("pipe")
    me = lax.axis_index("tensor")
    place = lax.axis_index("seq")
    tn = 256 if inner % 256 == 0 else LANES

    loads = [
        pltpu.make_async_copy(src.at[0], dst, w_sem.at[k])
        for k, (src, dst) in enumerate(
            (
                (inner_hbm, w_inner),
                (state_hbm, w_state),
                (step_hbm, w_step),
                (gate_hbm, w_gate),
                (out_hbm, w_out),
            )
        )
    ]

    def gather(m, j):
        return remote(
            u.at[m, me], u.at[m, me], ag_send.at[m, j], ag_recv.at[m, me], {"tensor": j}
        )

    def gathered(m, j):
        return remote(u.at[m, j], u.at[m, j], ag_send.at[m, j], ag_recv.at[m, j], {"tensor": j})

    def rim_copy(m):
        return remote(
            raw.at[m, pl.ds(rows - edge, edge)],
            rim.at[m],
            rim_send.at[m],
            rim_recv.at[m],
            {"seq": lax.rem(place + 1, n_seq)},
        )

    def chain(m, i):
        return remote(
            snd.at[m, i],
            ent.at[m, i],
            ch_send.at[m, i],
            ch_recv.at[m, i],
            {"seq": lax.rem(place + 1, n_seq)},
        )

    def part(m, j):
        return remote(
            term.at[m, j], parts.at[m, me], rs_send.at[m, j], rs_recv.at[m, me], {"tensor": j}
        )

    def parted(m, j):
        return remote(
            parts.at[m, j], parts.at[m, j], rs_send.at[m, j], rs_recv.at[m, j], {"tensor": j}
        )

    def squares(m, j):
        return remote(
            sq_own.at[m], sq_all.at[m, me], sq_send.at[m, j], sq_recv.at[m, me], {"tensor": j}
        )

    def squared(m, j):
        return remote(
            sq_all.at[m, j], sq_all.at[m, j], sq_send.at[m, j], sq_recv.at[m, j], {"tensor": j}
        )

    def relay(m):
        return remote(
            own.at[m],
            u.at[m, me],
            pipe_send.at[m],
            pipe_recv.at[m],
            {"pipe": lax.rem(section + 1, n_pipe)},
        )

    def others(action):
        for j in range(n_tensor):
            pl.when(me != j)(functools.partial(action, j))

    @pl.when(section == 0)
    def _():
        for m in range(micros):
            u[m, me] = tokens[m]
        for m in range(micros):
            others(lambda j, m=m: gather(m, j).start())

    for load in loads:
        load.start()

    taps[: reach + 2, :inner] = inner_taps[0]
    taps[: reach + 2, inner:] = state_taps[0]
    steps[...] = jnp.zeros_like(steps)
    rates[...] = jnp.zeros_like(rates)
    rates[0:1, :heads] = decay_rate[...]
    sq_acc[...] = jnp.zeros_like(sq_acc)

    @pl.when(place == 0)
    def _():
        rim[...] = jnp.zeros_like(rim)
        ent[...] = jnp.zeros_like(ent)

    low = lax.broadcasted_iota(jnp.int32, (rows, LANES), 0)
    lane = lax.broadcasted_iota(jnp.int32, (rows, LANES), 1)
    later = low >= lane

    def by_lane(values):
        result = values[0]
        for k in range(1, pack):
            result = jnp.where(lane >= k * head_size, values[k], result)
        return result

    def take_input(m):
        @pl.when(section > 0)
        def _():
            relay(m).wait_recv()
            others(lambda j: gather(m, j).start())

        others(lambda j: gathered(m, j).wait_recv())

        def norm(r, _):
            at = pl.ds(pl.multiple_of(r * 32, 32), 32)
            total = jnp.zeros((32, 1), F32)
            for j in range(n_tensor):
                v = u[m, j, at, :].astype(F32)
                total = total + jnp.sum(v * v, axis=1, keepdims=True)
            scale = lax.rsqrt(total / width + EPS)
            for j in range(n_tensor):
                cols = slice(j * narrow, (j + 1) * narrow)
                v = u[m, j, at, :].astype(F32)
                ni[m, at, cols] = (v * scale * prenorm[:, cols]).astype(BF16)
            return 0

        lax.fori_loop(0, rows // 32, norm, 0)

    def project(m):
        if m == 0:
            loads[0].wait()
            loads[1].wait()
            loads[2].wait()

        def tile(t, _):
            at = pl.ds(pl.multiple_of(t * tn, tn), tn)
            raw[m, :, at] = jnp.dot(
                ni[m], w_inner[:, at], preferred_element_type=F32
            ).astype(BF16)
            return 0

        lax.fori_loop(0, inner // tn, tile, 0)
        raw[m, :, inner:] = jnp.dot(ni[m], w_state[...], preferred_element_type=F32).astype(BF16)

        @pl.when(place < n_seq - 1)
        def _():
            rim_copy(m).start()

        step_raw = jnp.dot(ni[m], w_step[...], preferred_element_type=F32)
        v = step_raw + step_bias[...]
        steps[m, :, :heads] = jnp.maximum(v, 0.0) + jnp.log1p(jnp.exp(-jnp.abs(v)))
        step = steps[m]
        cum = jnp.dot(
            later.astype(F32),
            -step * rates[0:1],
            precision=lax.Precision.HIGHEST,
            preferred_element_type=F32,
        )
        cum_t[m] = cum.T
        step_t[m] = step.T

    def project_gate(m):
        if m == 0:
            loads[3].wait()

        def tile(t, _):
            at = pl.ds(pl.multiple_of(t * tn, tn), tn)
            gate[m, :, at] = jnp.dot(
                ni[m], w_gate[:, at], preferred_element_type=F32
            ).astype(BF16)
            return 0

        lax.fori_loop(0, inner // tn, tile, 0)

    def columns(m, i):
        crow, ccol, srow, scol = [], [], [], []
        for k in range(pack):
            h = i * pack + k
            c = jnp.broadcast_to(cum_t[m, pl.ds(h, 1), :], (LANES, rows))
            s = jnp.broadcast_to(step_t[m, pl.ds(h, 1), :], (LANES, rows))
            crow.append(c)
            srow.append(s)
            ccol.append(c.T)
            scol.append(s.T)
        return crow, ccol, srow, scol

    def convolve(m):
        @pl.when(place > 0)
        def _():
            rim_copy(m).wait_recv()

        def tile(t, _):
            at = pl.ds(pl.multiple_of(t * LANES, LANES), LANES)
            padded = jnp.concatenate([rim[m, :, at], raw[m, :, at]], axis=0).astype(F32)
            total = jnp.broadcast_to(taps[reach + 1 : reach + 2, at], (rows, LANES))
            for k in range(reach + 1):
                moved = padded if k == reach else pltpu.roll(padded, reach - k, 0)
                total = total + taps[k : k + 1, at] * moved[edge:]
            conv[m, t] = silu(total).astype(BF16)
            return 0

        lax.fori_loop(0, tiles, tile, 0)
        b = conv[m, pairs]
        b_t[m] = b.astype(F32).T.astype(BF16)
        scores[m] = lax.dot_general(
            conv[m, pairs + 1], b, (((1,), (1,)), ((), ())), preferred_element_type=F32
        )

        def state(i, _):
            _, ccol, _, scol = columns(m, i)
            c, s = by_lane(ccol), by_lane(scol)
            weighting = jnp.exp(c[rows - 1 :] - c) * s
            weighted = (conv[m, i].astype(F32) * weighting).astype(BF16)
            result = jnp.dot(b_t[m], weighted, preferred_element_type=F32)
            states[m, i] = result

            @pl.when(place == 0)
            def _():
                snd[m, i] = result.astype(BF16)
                chain(m, i).start()

            return 0

        lax.fori_loop(0, pairs, state, 0)

    def scan(m):
        def pair(i, _):
            crow, ccol, srow, _ = columns(m, i)
            c = by_lane(ccol)

            @pl.when(place > 0)
            def _():
                chain(m, i).wait_recv()

            entering = ent[m, i]

            @pl.when(jnp.logical_and(place > 0, place < n_seq - 1))
            def _():
                snd[m, i] = (
                    jnp.exp(c[rows - 1 :]) * entering.astype(F32) + states[m, i]
                ).astype(BF16)
                chain(m, i).start()

            x = conv[m, i]
            mixing = jnp.concatenate(
                [
                    (
                        scores[m]
                        * jnp.exp(jnp.where(later, ccol[k] - crow[k], -jnp.inf))
                        * srow[k]
                    ).astype(BF16)
                    for k in range(pack)
                ],
                axis=0,
            )
            inside = jnp.dot(mixing, x, preferred_element_type=F32)
            inside = by_lane([inside[k * rows : (k + 1) * rows] for k in range(pack)])
            across = jnp.dot(conv[m, pairs + 1], entering, preferred_element_type=F32)
            skip = by_lane(
                [jnp.full((rows, LANES), skip_scale[0, i * pack + k], F32) for k in range(pack)]
            )
            mixed = inside + jnp.exp(c) * across + skip * x.astype(F32)
            at = pl.ds(pl.multiple_of(i * LANES, LANES), LANES)
            gated = mixed * silu(gate[m, :, at].astype(F32))
            sq_acc[m] += gated * gated
            g[m, :, at] = (gated * inner_gain[:, at]).astype(BF16)
            return 0

        lax.fori_loop(0, pairs, pair, 0)

    def project_out(m):
        if m == 0:
            loads[4].wait()
        total = jnp.sum(sq_acc[m], axis=1, keepdims=True)
        sq_own[m] = jnp.broadcast_to(total, (rows, LANES)).T[:8]
        for j in range(n_tensor):
            term[m, j] = jnp.dot(
                g[m], w_out[:, j * narrow : (j + 1) * narrow], preferred_element_type=F32
            ).astype(BF16)

            @pl.when(me != j)
            def _():
                squares(m, j).start()
                part(m, j).start()

    def finish(m):
        parts[m, me] = term[m, me]
        sq_all[m, me] = sq_own[m]
        others(lambda j: squared(m, j).wait_recv())
        others(lambda j: parted(m, j).wait_recv())
        total = sq_all[m, 0]
        for j in range(1, n_tensor):
            total = total + sq_all[m, j]
        scale = lax.rsqrt(total / (inner * n_tensor) + EPS)
        sq_acc[m] = jnp.broadcast_to(scale[0:1], (LANES, rows)).T

        def add(r, _):
            at = pl.ds(pl.multiple_of(r * 32, 32), 32)
            summed = parts[m, 0, at, :].astype(F32)
            for j in range(1, n_tensor):
                summed = summed + parts[m, j, at, :].astype(F32)
            value = (u[m, me, at, :].astype(F32) + summed * sq_acc[m, at, 0:1]).astype(BF16)
            own[m, at, :] = value
            out[0, m, at, :] = value
            return 0

        lax.fori_loop(0, rows // 32, add, 0)

        @pl.when(section < n_pipe - 1)
        def _():
            relay(m).start()

    for m in range(micros):
        take_input(m)
        project(m)
        project_gate(m)
        convolve(m)
    for m in range(micros):
        scan(m)
        if m > 0:
            finish(m - 1)
        project_out(m)
    finish(micros - 1)

    def drain(m, _):
        others(lambda j: gather(m, j).wait_send())
        others(lambda j: part(m, j).wait_send())
        others(lambda j: squares(m, j).wait_send())

        @pl.when(place < n_seq - 1)
        def _():
            rim_copy(m).wait_send()

            def one(i, _):
                chain(m, i).wait_send()
                return 0

            lax.fori_loop(0, pairs, one, 0)

        @pl.when(section < n_pipe - 1)
        def _():
            relay(m).wait_send()

        return 0

    lax.fori_loop(0, micros, drain, 0)


def shards(sizes, *args):
    tokens, prenorm, gate_w, inner_w, state_w, step_w = args[:6]
    n_pipe, n_tensor, n_seq = sizes
    micros, rows, narrow = tokens.shape
    width = prenorm.shape[1]
    inner = inner_w.shape[2]
    maps = state_w.shape[2]
    heads = step_w.shape[2]
    pairs = inner // LANES
    wide = inner + maps
    edge = 16
    vmem = pl.BlockSpec(memory_space=pltpu.VMEM)
    far = pl.BlockSpec(memory_space=pl.ANY)
    smem = pl.BlockSpec(memory_space=pltpu.SMEM)
    dma = pltpu.SemaphoreType.DMA
    V = pltpu.VMEM
    return pl.pallas_call(
        functools.partial(kernel, sizes),
        out_shape=jax.ShapeDtypeStruct((1, micros, rows, narrow), BF16),
        in_specs=[vmem, vmem, far, far, far, far, vmem, vmem, vmem, vmem, smem, vmem, far],
        out_specs=vmem,
        scratch_shapes=[
            V((width, inner), BF16),
            V((width, inner), BF16),
            V((width, maps), BF16),
            V((width, heads), BF16),
            V((inner, width), BF16),
            V((micros, n_tensor, rows, narrow), BF16),
            V((micros, rows, width), BF16),
            V((micros, rows, wide), BF16),
            V((micros, edge, wide), BF16),
            V((8, wide), F32),
            V((micros, wide // LANES, rows, LANES), BF16),
            V((micros, rows, inner), BF16),
            V((micros, rows, LANES), F32),
            V((8, LANES), F32),
            V((micros, LANES, rows), F32),
            V((micros, LANES, rows), F32),
            V((micros, LANES, rows), BF16),
            V((micros, rows, rows), F32),
            V((micros, pairs, LANES, LANES), F32),
            V((micros, pairs, LANES, LANES), BF16),
            V((micros, pairs, LANES, LANES), BF16),
            V((micros, rows, inner), BF16),
            V((micros, rows, LANES), F32),
            V((micros, 8, rows), F32),
            V((micros, n_tensor, 8, rows), F32),
            V((micros, n_tensor, rows, narrow), BF16),
            V((micros, n_tensor, rows, narrow), BF16),
            V((micros, rows, narrow), BF16),
            dma((5,)),
            dma((micros, n_tensor)),
            dma((micros, n_tensor)),
            dma((micros,)),
            dma((micros,)),
            dma((micros, pairs)),
            dma((micros, pairs)),
            dma((micros, n_tensor)),
            dma((micros, n_tensor)),
            dma((micros, n_tensor)),
            dma((micros, n_tensor)),
            dma((micros,)),
            dma((micros,)),
        ],
        compiler_params=pltpu.CompilerParams(
            has_side_effects=True, vmem_limit_bytes=60000 * 1024
        ),
    )(*args)


def solution(mesh):
    sizes = (mesh.shape["pipe"], mesh.shape["tensor"], mesh.shape["seq"])
    placed = (
        P(None, "seq", "tensor"),
        P("pipe", None),
        P("pipe", None, "tensor"),
        P("pipe", None, "tensor"),
        P("pipe", None, None),
        P("pipe", None, "tensor"),
        P("pipe", None, "tensor"),
        P("pipe", None, None),
        P("pipe", "tensor"),
        P("pipe", "tensor"),
        P("pipe", "tensor"),
        P("pipe", "tensor"),
        P("pipe", "tensor", None),
    )
    return jax.shard_map(
        functools.partial(shards, sizes),
        mesh=mesh,
        in_specs=placed,
        out_specs=P("pipe", None, "seq", "tensor"),
        check_vma=False,
    )
```

```python
import functools

import jax
import jax.numpy as jnp
from jax import lax
from jax.experimental import pallas as pl
from jax.experimental.pallas import tpu as pltpu
from jax.sharding import PartitionSpec as P

EPS = 1e-05
LANES = 128
MESH = pl.DeviceIdType.MESH
F32 = jnp.float32
BF16 = jnp.bfloat16


def silu(v):
    return v / (1.0 + jnp.exp(-v))


def remote(src, dst, send, recv, where):
    return pltpu.make_async_remote_copy(
        src_ref=src, dst_ref=dst, send_sem=send, recv_sem=recv, device_id=where, device_id_type=MESH
    )


def kernel(
    sizes,
    tokens,
    prenorm_hbm,
    gate_hbm,
    inner_hbm,
    state_hbm,
    step_hbm,
    inner_taps_hbm,
    state_taps_hbm,
    step_bias_hbm,
    decay_rate_hbm,
    skip_scale_hbm,
    inner_gain_hbm,
    out_hbm,
    out,
    prenorm,
    inner_taps,
    state_taps,
    step_bias,
    decay_rate,
    skip_scale,
    inner_gain,
    w_gate,
    w_inner,
    w_state,
    w_step,
    w_out,
    u,
    ni,
    raw,
    rim,
    skip_t,
    conv,
    gate,
    steps,
    rates,
    cum_t,
    step_t,
    b_t,
    scores,
    states,
    ent,
    snd,
    g,
    sq_acc,
    sq_own,
    sq_all,
    term,
    parts,
    own,
    w_sem,
    v_sem,
    t_sem,
    ag_send,
    ag_recv,
    rim_send,
    rim_recv,
    ch_send,
    ch_recv,
    rs_send,
    rs_recv,
    sq_send,
    sq_recv,
    pipe_send,
    pipe_recv,
):
    n_pipe, n_tensor, n_seq = sizes
    micros, rows, narrow = own.shape
    width = prenorm.shape[1]
    inner = w_inner.shape[1]
    heads = step_bias.shape[1]
    head_size = inner // heads
    pack = LANES // head_size
    pairs = inner // LANES
    tiles = raw.shape[2] // LANES
    reach = inner_taps.shape[0] - 2
    edge = rim.shape[1]
    section = lax.axis_index("pipe")
    me = lax.axis_index("tensor")
    place = lax.axis_index("seq")
    tn = 256 if inner % 256 == 0 else LANES

    loads = [
        pltpu.make_async_copy(src.at[0], dst, w_sem.at[k])
        for k, (src, dst) in enumerate(
            (
                (inner_hbm, w_inner),
                (state_hbm, w_state),
                (step_hbm, w_step),
                (gate_hbm, w_gate),
                (out_hbm, w_out),
            )
        )
    ]
    vectors = [
        pltpu.make_async_copy(src, dst, v_sem.at[k])
        for k, (src, dst) in enumerate(
            (
                (prenorm_hbm, prenorm),
                (inner_taps_hbm, inner_taps),
                (state_taps_hbm, state_taps),
                (step_bias_hbm, step_bias),
                (decay_rate_hbm, decay_rate),
                (skip_scale_hbm, skip_scale),
                (inner_gain_hbm, inner_gain),
            )
        )
    ]

    def stage(m):
        return pltpu.make_async_copy(tokens.at[m], u.at[m, me], t_sem.at[m])

    core = lax.rem(me, 2)
    partner = me + 1 - 2 * core
    chips = n_tensor // 2
    pieces = ag_send.shape[2]
    some = rows // pieces

    def at_chip(d):
        return 2 * lax.rem(me // 2 + d, chips) + core

    def gather(m, q, src, key, where):
        block = u.at[m, src, pl.ds(q * some, some)]
        return remote(
            block, block, ag_send.at[m, key, q], ag_recv.at[m, src, q], {"tensor": where}
        )

    def near(m, q):
        return gather(m, q, me, partner, partner)

    def cross(m, d, q):
        return gather(m, q, me, at_chip(d), at_chip(d))

    def hand(m, d, q):
        return gather(m, q, at_chip(d), at_chip(d) + 1 - 2 * core, partner)

    def gathered(m, q, src):
        return gather(m, q, src, src, partner)

    def send_own(m, q):
        for d in range(1, chips):
            cross(m, d, q).start()
        near(m, q).start()

    def rim_copy(m):
        return remote(
            raw.at[m, pl.ds(rows - edge, edge)],
            rim.at[m],
            rim_send.at[m],
            rim_recv.at[m],
            {"seq": lax.rem(place + 1, n_seq)},
        )

    def chain(m, i):
        return remote(
            snd.at[m, i],
            ent.at[m, i],
            ch_send.at[m, i],
            ch_recv.at[m, i],
            {"seq": lax.rem(place + 1, n_seq)},
        )

    def part(m, j):
        return remote(
            term.at[m, j], parts.at[m, me], rs_send.at[m, j], rs_recv.at[m, me], {"tensor": j}
        )

    def parted(m, j):
        return remote(
            parts.at[m, j], parts.at[m, j], rs_send.at[m, j], rs_recv.at[m, j], {"tensor": j}
        )

    def squares(m, j):
        return remote(
            sq_own.at[m], sq_all.at[m, me], sq_send.at[m, j], sq_recv.at[m, me], {"tensor": j}
        )

    def squared(m, j):
        return remote(
            sq_all.at[m, j], sq_all.at[m, j], sq_send.at[m, j], sq_recv.at[m, j], {"tensor": j}
        )

    def relay(m, q):
        return remote(
            own.at[m, pl.ds(q * some, some)],
            u.at[m, me, pl.ds(q * some, some)],
            pipe_send.at[m, q],
            pipe_recv.at[m, q],
            {"pipe": lax.rem(section + 1, n_pipe)},
        )

    def others(action):
        for j in range(n_tensor):
            pl.when(me != j)(functools.partial(action, j))

    @pl.when(section == 0)
    def _():
        for m in range(micros):
            stage(m).start()

    for load in vectors + loads:
        load.start()

    barrier = pltpu.get_barrier_semaphore()

    def greet(where):
        pl.semaphore_signal(barrier, inc=1, device_id=where, device_id_type=MESH)

    others(lambda j: greet({"tensor": j}))
    partners = n_tensor - 1
    for axis, index, count in (("seq", place, n_seq), ("pipe", section, n_pipe)):
        pl.when(index > 0)(functools.partial(greet, {axis: index - 1}))
        pl.when(index < count - 1)(functools.partial(greet, {axis: index + 1}))
        partners = partners + jnp.where(index > 0, 1, 0) + jnp.where(index < count - 1, 1, 0)
    pl.semaphore_wait(barrier, partners)

    @pl.when(section == 0)
    def _():
        for m in range(micros):
            stage(m).wait()
        for q in range(pieces):
            send_own(0, q)

    for load in vectors:
        load.wait()
    steps[...] = jnp.zeros_like(steps)
    rates[...] = jnp.zeros_like(rates)
    rates[0:1, :heads] = decay_rate[...]
    rates[1:2, :heads] = skip_scale[...]
    skip_t[...] = jnp.broadcast_to(rates[1:2], (rows, LANES)).T
    sq_acc[...] = jnp.zeros_like(sq_acc)

    @pl.when(place == 0)
    def _():
        rim[...] = jnp.zeros_like(rim)
        ent[...] = jnp.zeros_like(ent)

    low = lax.broadcasted_iota(jnp.int32, (rows, LANES), 0)
    lane = lax.broadcasted_iota(jnp.int32, (rows, LANES), 1)
    later = low >= lane

    def by_lane(values):
        result = values[0]
        for k in range(1, pack):
            result = jnp.where(lane >= k * head_size, values[k], result)
        return result

    def forward(m):
        for q in range(pieces):
            relay(m, q).wait_recv()
            send_own(m, q)

    def hand_over(m):
        for q in range(pieces):
            for d in range(1, chips):
                gathered(m, q, at_chip(d)).wait_recv()
                hand(m, d, q).start()

    def take_input(m):
        for q in range(pieces):
            gathered(m, q, partner).wait_recv()
            for d in range(1, chips):
                gathered(m, q, at_chip(d) + 1 - 2 * core).wait_recv()

        def norm(r, _):
            at = pl.ds(pl.multiple_of(r * 32, 32), 32)
            total = jnp.zeros((32, 1), F32)
            for j in range(n_tensor):
                v = u[m, j, at, :].astype(F32)
                total = total + jnp.sum(v * v, axis=1, keepdims=True)
            scale = lax.rsqrt(total / width + EPS)
            for j in range(n_tensor):
                cols = slice(j * narrow, (j + 1) * narrow)
                v = u[m, j, at, :].astype(F32)
                ni[m, at, cols] = (v * scale * prenorm[:, cols]).astype(BF16)
            return 0

        lax.fori_loop(0, rows // 32, norm, 0)

    def project(m):
        if m == 0:
            loads[0].wait()
            loads[1].wait()
            loads[2].wait()

        def tile(t, _):
            at = pl.ds(pl.multiple_of(t * tn, tn), tn)
            raw[m, :, at] = jnp.dot(
                ni[m], w_inner[:, at], preferred_element_type=F32
            ).astype(BF16)
            return 0

        lax.fori_loop(0, inner // tn, tile, 0)
        raw[m, :, inner:] = jnp.dot(ni[m], w_state[...], preferred_element_type=F32).astype(BF16)

        @pl.when(place < n_seq - 1)
        def _():
            rim_copy(m).start()

        step_raw = lax.dot_general(
            ni[m], w_step[...], (((1,), (1,)), ((), ())), preferred_element_type=F32
        )
        v = step_raw + step_bias[...]
        steps[m, :, :heads] = jnp.maximum(v, 0.0) + jnp.log1p(jnp.exp(-jnp.abs(v)))
        step = steps[m]
        cum = jnp.dot(
            later.astype(F32),
            -step * rates[0:1],
            precision=lax.Precision.HIGHEST,
            preferred_element_type=F32,
        )
        cum_t[m] = cum.T
        step_t[m] = step.T

    def project_gate(m):
        if m == 0:
            loads[3].wait()

        def tile(t, _):
            at = pl.ds(pl.multiple_of(t * tn, tn), tn)
            gate[m, :, at] = jnp.dot(
                ni[m], w_gate[:, at], preferred_element_type=F32
            ).astype(BF16)
            return 0

        lax.fori_loop(0, inner // tn, tile, 0)

    def columns(m, i):
        crow, ccol, srow, scol = [], [], [], []
        for k in range(pack):
            h = i * pack + k
            c = jnp.broadcast_to(cum_t[m, pl.ds(h, 1), :], (LANES, rows))
            s = jnp.broadcast_to(step_t[m, pl.ds(h, 1), :], (LANES, rows))
            crow.append(c)
            srow.append(s)
            ccol.append(c.T)
            scol.append(s.T)
        return crow, ccol, srow, scol

    def convolve(m):
        @pl.when(place > 0)
        def _():
            rim_copy(m).wait_recv()

        def tile(taps, first, t, _):
            at = pl.ds(pl.multiple_of(t * LANES, LANES), LANES)
            tap = pl.ds(pl.multiple_of((t - first) * LANES, LANES), LANES)
            padded = jnp.concatenate([rim[m, :, at], raw[m, :, at]], axis=0).astype(F32)
            total = jnp.broadcast_to(taps[reach + 1, :, tap], (rows, LANES))
            for k in range(reach + 1):
                moved = padded if k == reach else pltpu.roll(padded, reach - k, 0)
                total = total + taps[k, :, tap] * moved[edge:]
            conv[m, t] = silu(total).astype(BF16)
            return 0

        lax.fori_loop(0, pairs, functools.partial(tile, inner_taps, 0), 0)
        lax.fori_loop(pairs, tiles, functools.partial(tile, state_taps, pairs), 0)
        b = conv[m, pairs]
        b_t[m] = b.astype(F32).T.astype(BF16)
        scores[m] = lax.dot_general(
            conv[m, pairs + 1], b, (((1,), (1,)), ((), ())), preferred_element_type=F32
        )

        def state(i, _):
            _, ccol, _, scol = columns(m, i)
            c, s = by_lane(ccol), by_lane(scol)
            weighting = jnp.exp(c[rows - 1 :] - c) * s
            weighted = (conv[m, i].astype(F32) * weighting).astype(BF16)
            result = jnp.dot(b_t[m], weighted, preferred_element_type=F32)
            states[m, i] = result

            @pl.when(place == 0)
            def _():
                snd[m, i] = result.astype(BF16)
                chain(m, i).start()

            return 0

        lax.fori_loop(0, pairs, state, 0)

    def scan(m):
        def pair(i, _):
            crow, ccol, srow, _ = columns(m, i)
            c = by_lane(ccol)

            @pl.when(place > 0)
            def _():
                chain(m, i).wait_recv()

            entering = ent[m, i]

            @pl.when(jnp.logical_and(place > 0, place < n_seq - 1))
            def _():
                snd[m, i] = (
                    jnp.exp(c[rows - 1 :]) * entering.astype(F32) + states[m, i]
                ).astype(BF16)
                chain(m, i).start()

            x = conv[m, i]
            mixing = jnp.concatenate(
                [
                    (
                        scores[m]
                        * jnp.exp(jnp.where(later, ccol[k] - crow[k], -jnp.inf))
                        * srow[k]
                    ).astype(BF16)
                    for k in range(pack)
                ],
                axis=0,
            )
            inside = jnp.dot(mixing, x, preferred_element_type=F32)
            inside = by_lane([inside[k * rows : (k + 1) * rows] for k in range(pack)])
            across = jnp.dot(conv[m, pairs + 1], entering, preferred_element_type=F32)
            skip = by_lane(
                [
                    jnp.broadcast_to(skip_t[pl.ds(i * pack + k, 1), :], (rows, LANES))
                    for k in range(pack)
                ]
            )
            mixed = inside + jnp.exp(c) * across + skip * x.astype(F32)
            at = pl.ds(pl.multiple_of(i * LANES, LANES), LANES)
            gated = mixed * silu(gate[m, :, at].astype(F32))
            sq_acc[m] += gated * gated
            g[m, :, at] = (gated * inner_gain[:, at]).astype(BF16)
            return 0

        lax.fori_loop(0, pairs, pair, 0)

    def project_out(m):
        if m == 0:
            loads[4].wait()
        total = jnp.sum(sq_acc[m], axis=1, keepdims=True)
        sq_own[m] = jnp.broadcast_to(total, (rows, LANES)).T[:8]
        for j in range(n_tensor):
            term[m, j] = jnp.dot(
                g[m], w_out[:, j * narrow : (j + 1) * narrow], preferred_element_type=F32
            ).astype(BF16)

            @pl.when(me != j)
            def _():
                squares(m, j).start()
                part(m, j).start()

    def finish(m):
        parts[m, me] = term[m, me]
        sq_all[m, me] = sq_own[m]
        others(lambda j: squared(m, j).wait_recv())
        others(lambda j: parted(m, j).wait_recv())
        total = sq_all[m, 0]
        for j in range(1, n_tensor):
            total = total + sq_all[m, j]
        scale = lax.rsqrt(total / (inner * n_tensor) + EPS)
        sq_acc[m] = jnp.broadcast_to(scale[0:1], (LANES, rows)).T

        def add(r, _):
            at = pl.ds(pl.multiple_of(r * 32, 32), 32)
            summed = parts[m, 0, at, :].astype(F32)
            for j in range(1, n_tensor):
                summed = summed + parts[m, j, at, :].astype(F32)
            value = (u[m, me, at, :].astype(F32) + summed * sq_acc[m, at, 0:1]).astype(BF16)
            own[m, at, :] = value
            out[0, m, at, :] = value
            return 0

        for q in range(pieces):
            lax.fori_loop(q * some // 32, (q + 1) * some // 32, add, 0)

            @pl.when(section < n_pipe - 1)
            def _():
                relay(m, q).start()

    @pl.when(section == 0)
    def _():
        hand_over(0)
        for m in range(1, micros):
            for q in range(pieces):
                send_own(m, q)
        take_input(0)
        project(0)
        project_gate(0)
        for m in range(1, micros):
            hand_over(m)
        convolve(0)
        for m in range(micros):
            if m + 1 < micros:
                take_input(m + 1)
                project(m + 1)
            if m > 0:
                finish(m - 1)
            scan(m)
            project_out(m)
            if m + 1 < micros:
                convolve(m + 1)
                project_gate(m + 1)
        finish(micros - 1)

    @pl.when(section > 0)
    def _():
        forward(0)
        hand_over(0)
        take_input(0)
        project(0)
        project_gate(0)
        convolve(0)
        for m in range(micros):
            if m + 1 < micros:
                forward(m + 1)
            if m > 0:
                finish(m - 1)
            scan(m)
            if m + 1 < micros:
                hand_over(m + 1)
            project_out(m)
            if m + 1 < micros:
                take_input(m + 1)
                project(m + 1)
                project_gate(m + 1)
                convolve(m + 1)
        finish(micros - 1)

    def drain(m, _):
        for q in range(pieces):
            near(m, q).wait_send()
            for d in range(1, chips):
                cross(m, d, q).wait_send()
                hand(m, d, q).wait_send()
        others(lambda j: part(m, j).wait_send())
        others(lambda j: squares(m, j).wait_send())

        @pl.when(place < n_seq - 1)
        def _():
            rim_copy(m).wait_send()

            def one(i, _):
                chain(m, i).wait_send()
                return 0

            lax.fori_loop(0, pairs, one, 0)

        @pl.when(section < n_pipe - 1)
        def _():
            for q in range(pieces):
                relay(m, q).wait_send()

        return 0

    lax.fori_loop(0, micros, drain, 0)


def shards(sizes, *args):
    tokens, prenorm, gate_w, inner_w, state_w, step_w = args[:6]
    n_pipe, n_tensor, n_seq = sizes
    micros, rows, narrow = tokens.shape
    width = prenorm.shape[1]
    inner = inner_w.shape[2]
    maps = state_w.shape[2]
    heads = step_w.shape[2]
    pairs = inner // LANES
    wide = inner + maps
    step_w = jnp.swapaxes(step_w, 1, 2)
    inner_taps, state_taps = (jnp.swapaxes(a, 0, 1) for a in args[6:8])
    args = (tokens, prenorm, gate_w, inner_w, state_w, step_w, inner_taps, state_taps) + args[8:]
    edge = 16
    vmem = pl.BlockSpec(memory_space=pltpu.VMEM)
    far = pl.BlockSpec(memory_space=pl.ANY)
    dma = pltpu.SemaphoreType.DMA
    V = pltpu.VMEM
    return pl.pallas_call(
        functools.partial(kernel, sizes),
        out_shape=jax.ShapeDtypeStruct((1, micros, rows, narrow), BF16),
        in_specs=[far] * len(args),
        out_specs=vmem,
        scratch_shapes=[
            V((1, width), F32),
            V(inner_taps.shape, F32),
            V(state_taps.shape, F32),
            V((1, heads), F32),
            V((1, heads), F32),
            V((1, heads), F32),
            V((1, inner), F32),
            V((width, inner), BF16),
            V((width, inner), BF16),
            V((width, maps), BF16),
            V((heads, width), BF16),
            V((inner, width), BF16),
            V((micros, n_tensor, rows, narrow), BF16),
            V((micros, rows, width), BF16),
            V((micros, rows, wide), BF16),
            V((micros, edge, wide), BF16),
            V((LANES, rows), F32),
            V((micros, wide // LANES, rows, LANES), BF16),
            V((micros, rows, inner), BF16),
            V((micros, rows, LANES), F32),
            V((8, LANES), F32),
            V((micros, LANES, rows), F32),
            V((micros, LANES, rows), F32),
            V((micros, LANES, rows), BF16),
            V((micros, rows, rows), F32),
            V((micros, pairs, LANES, LANES), F32),
            V((micros, pairs, LANES, LANES), BF16),
            V((micros, pairs, LANES, LANES), BF16),
            V((micros, rows, inner), BF16),
            V((micros, rows, LANES), F32),
            V((micros, 8, rows), F32),
            V((micros, n_tensor, 8, rows), F32),
            V((micros, n_tensor, rows, narrow), BF16),
            V((micros, n_tensor, rows, narrow), BF16),
            V((micros, rows, narrow), BF16),
            dma((5,)),
            dma((7,)),
            dma((micros,)),
            dma((micros, n_tensor, 2)),
            dma((micros, n_tensor, 2)),
            dma((micros,)),
            dma((micros,)),
            dma((micros, pairs)),
            dma((micros, pairs)),
            dma((micros, n_tensor)),
            dma((micros, n_tensor)),
            dma((micros, n_tensor)),
            dma((micros, n_tensor)),
            dma((micros, 2)),
            dma((micros, 2)),
        ],
        compiler_params=pltpu.CompilerParams(
            collective_id=0, has_side_effects=True, vmem_limit_bytes=60000 * 1024
        ),
    )(*args)


def solution(mesh):
    sizes = (mesh.shape["pipe"], mesh.shape["tensor"], mesh.shape["seq"])
    placed = (
        P(None, "seq", "tensor"),
        P("pipe", None),
        P("pipe", None, "tensor"),
        P("pipe", None, "tensor"),
        P("pipe", None, None),
        P("pipe", None, "tensor"),
        P("pipe", None, "tensor"),
        P("pipe", None, None),
        P("pipe", "tensor"),
        P("pipe", "tensor"),
        P("pipe", "tensor"),
        P("pipe", "tensor"),
        P("pipe", "tensor", None),
    )
    return jax.shard_map(
        functools.partial(shards, sizes),
        mesh=mesh,
        in_specs=placed,
        out_specs=P("pipe", None, "seq", "tensor"),
        check_vma=False,
    )
```
